32 devices in a mesh: layer: 8 (over y, x, core), row: 4 (over z).
Axes of the slice: x: 2, y: 2, z: 4, core: 2. Of those that a mesh axis runs over, the one named last changes fastest.
Arguments:
- magnet: float32 [3, 8, 1024, 1024], P(None, 'layer', 'row'), may hold values from -1 to 1, as said below
- saturation: float32 [8], P('layer'), may hold values from 0.5 to 2
- stiffness: float32 [8], P('layer'), may hold values from 0.1 to 0.4
- damping: float32 [8], P('layer'), may hold values from 0.02 to 0.5
- interface_sign: int32 [8, 2], P('layer'), may hold values from -1 to 1, as said below
Outputs:
- torque: float32 [3, 8, 1024, 1024], P(None, 'layer', 'row')
The draws below stay inside these ranges and needn't reach their ends.
Inputs may be any that keep to these rules, and one draw needn't show every extreme that they name: `magnet`: the three components of every cell form a unit vector. Every entry is -1 or 1; interface_sign[l, 1] equals interface_sign[l + 1, 0], the sign of the interface between layers l and l + 1; interface_sign[0, 0] and interface_sign[7, 1] belong to no interface.
All inputs are finite; a program needn't handle non-finite values.
Results may differ from the reference program's by a relative error of at most 0.0003.
Values sent between devices are 32-bit elements; how exact they have to be, the bound alone decides.
A program may use at most 128 MiB of HBM per device.

```python
import math
import jax
import jax.numpy as jnp
from jax import lax

NX = 1024
NY = 1024
LAYERS = 8


def draw_magnet(key, part):
    raw_field = jax.random.normal(key, (3, LAYERS, NY, NX), jnp.float32)
    return raw_field / jnp.sqrt(jnp.sum(raw_field * raw_field, axis=0, keepdims=True) + 1e-12)


def draw_interface_sign(key, part):
    coin_bits = jax.random.randint(jax.random.fold_in(key, 7), (LAYERS + 1,), 0, 2)
    values = 2 * coin_bits - 1
    return jnp.stack([values[:-1], values[1:]], axis=1).astype(jnp.int32)


def block_levels(own_key, dims, split, smallest, high):
    factor_of = 1.0
    for dim, blocks in split:
        heights = jax.random.uniform(jax.random.fold_in(jax.random.fold_in(own_key, 6), dim), (blocks,), jnp.float32, smallest / len(split), high / len(split))
        factor_of = factor_of * jnp.repeat(jnp.exp(heights), dims[dim] // blocks).reshape((-1,) + (1,) * (len(dims) - 1 - dim))
    return factor_of


def setup_inputs(seed: int = 0) -> dict:
    key_list = jax.random.split(jax.random.key(seed), 6)
    return {
        "magnet": draw_magnet(jax.random.fold_in(key_list[5], 71), 0),
        "saturation": jnp.clip(jnp.exp(math.log(2.0) - 1.3862944 * jax.random.uniform(key_list[1], (LAYERS,), jnp.float32) ** block_levels(key_list[1], (LAYERS,), ((0, 8),), -0.2, 0.2)), 0.5, 2.0),
        "stiffness": jnp.clip(jnp.exp(math.log(0.4) - 1.3862944 * jax.random.uniform(key_list[2], (LAYERS,), jnp.float32) ** block_levels(key_list[2], (LAYERS,), ((0, 8),), -0.2, 0.2)), 0.1, 0.4),
        "damping": jnp.clip(jnp.exp(math.log(0.5) - 3.218876 * jax.random.uniform(key_list[3], (LAYERS,), jnp.float32) ** block_levels(key_list[3], (LAYERS,), ((0, 8),), -0.2, 0.2)), 0.02, 0.5),
        "interface_sign": draw_interface_sign(jax.random.fold_in(key_list[5], 71), 0),
    }


THICKNESS = 1.0
LAYER_PITCH = 1.5
RKKY_STRENGTH = 0.8

def wave_numbers(length):
    position = jnp.arange(length, dtype=jnp.int32)
    position = jnp.where(position < length // 2, position, position - length)
    return 2.0 * jnp.pi / length * position.astype(jnp.float32)

def cross_product(vector_one, vector_two):
    return jnp.stack([vector_one[1] * vector_two[2] - vector_one[2] * vector_two[1], vector_one[2] * vector_two[0] - vector_one[0] * vector_two[2], vector_one[0] * vector_two[1] - vector_one[1] * vector_two[0]])

def reference(magnet, saturation, stiffness, damping, interface_sign):
    wave_y = wave_numbers(NY)[:, None]
    wave_x = wave_numbers(NX)[None, :]
    square = wave_x * wave_x + wave_y * wave_y
    anchor = square == 0.0
    wave_norm = jnp.sqrt(jnp.where(anchor, 1.0, square))
    unit_x = jnp.where(anchor, 0.0, wave_x / wave_norm)
    unit_y = jnp.where(anchor, 0.0, wave_y / wave_norm)
    self_z = jnp.where(anchor, 1.0, -jnp.expm1(-THICKNESS * wave_norm) / (THICKNESS * wave_norm))
    form_factor = jnp.where(anchor, 0.0, jnp.expm1(-THICKNESS * wave_norm) ** 2 / (2.0 * THICKNESS * wave_norm))
    spectra = jnp.fft.fft2(magnet * saturation[None, :, None, None], axes=(2, 3))
    along_wave = unit_x * spectra[0] + unit_y * spectra[1]
    normal = spectra[2]
    layer_ids = jnp.arange(LAYERS, dtype=jnp.int32)

    def one_layer(target):
        layer_gap = target - layer_ids
        distance = jnp.abs(layer_gap).astype(jnp.float32)[:, None, None]
        gap_sign = jnp.sign(layer_gap).astype(jnp.float32)[:, None, None]
        weight = jnp.where((layer_gap == 0)[:, None, None], 0.0, form_factor * jnp.exp(-wave_norm * (LAYER_PITCH * distance - THICKNESS)))
        psi_part = lax.optimization_barrier(jnp.sum(weight * (along_wave - 1j * gap_sign * normal), axis=0))
        chi_part = lax.optimization_barrier(jnp.sum(weight * (normal + 1j * gap_sign * along_wave), axis=0))
        return (psi_part, chi_part)
    psi_sum, chi_sum = lax.map(one_layer, layer_ids)
    psi_total = psi_sum + (1.0 - self_z) * along_wave
    chi_total = chi_sum + self_z * normal
    field_spectra = jnp.stack([-unit_x * psi_total, -unit_y * psi_total, -chi_total])
    demag_field = jnp.real(jnp.fft.ifft2(field_spectra, axes=(2, 3)))
    laplace = jnp.roll(magnet, 1, 2) + jnp.roll(magnet, -1, 2) + jnp.roll(magnet, 1, 3) + jnp.roll(magnet, -1, 3) - 4.0 * magnet
    exchange_field = stiffness[None, :, None, None] * laplace
    zero_layer = jnp.zeros_like(magnet[:, :1])
    layer_below = jnp.concatenate([zero_layer, magnet[:, :-1]], axis=1)
    layer_above = jnp.concatenate([magnet[:, 1:], zero_layer], axis=1)
    sign_value = interface_sign.astype(jnp.float32)
    rkky_field = RKKY_STRENGTH * (sign_value[None, :, 0, None, None] * layer_below + sign_value[None, :, 1, None, None] * layer_above)
    total_field = demag_field + exchange_field + rkky_field
    precess = cross_product(magnet, total_field)
    relax_term = cross_product(magnet, precess)
    damping_now = damping[None, :, None, None]
    return -(precess + damping_now * relax_term) / (1.0 + damping_now * damping_now)
```

```python
import functools
import math

import jax
import jax.numpy as jnp
import numpy as np
from jax import lax
from jax.experimental import pallas as pl
from jax.experimental.pallas import tpu as pltpu
from jax.sharding import PartitionSpec as P

THICKNESS = 1.0
LAYER_PITCH = 1.5
RKKY_STRENGTH = 0.8
HIGH = lax.Precision.HIGH
LANES = 128


def angle_pair(phase):
    return np.cos(phase).astype(np.float32), np.sin(phase).astype(np.float32)


def turn(first, second, modulus):
    return 2.0 * math.pi / modulus * (np.outer(first, second) % modulus)


def outer_cosine(angle_one, angle_two):
    cos_one, sin_one = angle_pair(angle_one)
    cos_two, sin_two = angle_pair(angle_two)
    table = cos_one[:, None] * jnp.asarray(cos_two)[None] - sin_one[:, None] * jnp.asarray(sin_two)[None]
    return table.reshape(-1, table.shape[2])


def x_table(length, devices):
    width = length // 2 // devices
    points = np.arange(length)
    base = turn(width * np.arange(devices), points, length)
    step = turn(np.arange(width), points, length)
    table = outer_cosine(base, np.concatenate([step, step + math.pi / 2]))
    rows = lax.broadcasted_iota(jnp.int32, table.shape, 0)
    odd = lax.broadcasted_iota(jnp.int32, table.shape, 1) % 2
    return jnp.where(rows == width, 1.0 - 2.0 * odd.astype(jnp.float32), table)


def y_table(length):
    freq = np.arange(length).reshape(-1, 1, LANES)
    freq = np.broadcast_to(freq, (length // LANES, 2, LANES)).reshape(-1)
    shift = np.broadcast_to(np.array([0.0, math.pi / 2])[None, :, None], (length // LANES, 2, LANES)).reshape(-1)
    fine = 32
    coarse = turn(fine * np.arange(length // fine), freq, length) - shift[None]
    return outer_cosine(coarse, turn(np.arange(fine), freq, length))


def plane(wave_x, wave_y):
    square = wave_x * wave_x + wave_y * wave_y
    anchor = square == 0.0
    norm = jnp.sqrt(jnp.where(anchor, 1.0, square))
    unit_x = jnp.where(anchor, 0.0, wave_x / norm)
    unit_y = jnp.where(anchor, 0.0, wave_y / norm)
    depth = THICKNESS * norm
    series = 1.0 - depth / 11.0
    for term in range(10, 2, -1):
        series = 1.0 - depth / term * series
    rest = jnp.where(depth < 0.5, 0.5 * depth * series, 1.0 - (1.0 - jnp.exp(-depth)) / depth)
    rest = jnp.where(anchor, 0.0, rest)
    self_z = 1.0 - rest
    form = jnp.where(anchor, 0.0, 0.5 * depth * self_z * self_z)
    near = form * jnp.exp(-norm * (LAYER_PITCH - THICKNESS))
    decay = jnp.exp(-norm * LAYER_PITCH)
    laplace = 2.0 * jnp.cos(wave_x) + 2.0 * jnp.cos(wave_y) - 4.0
    return unit_x, unit_y, rest, self_z, near, decay, laplace


def field_of(spectra, factors, sign_x, sign_y, params, layers):
    unit_x, unit_y, rest, self_z, near, decay, laplace = factors
    unit_x = unit_x * sign_x
    unit_y = unit_y * sign_y
    along, normal, up, down = [], [], [], []
    for l in range(layers):
        moment = params[l, 0]
        along.append([moment * (unit_x * spectra[l][0][i] + unit_y * spectra[l][1][i]) for i in range(2)])
        normal.append([moment * spectra[l][2][i] for i in range(2)])
    zero = jnp.zeros_like(along[0][0])
    carry = [zero, zero]
    for l in range(layers):
        up.append(carry)
        carry = [
            along[l][0] + normal[l][1] + decay * carry[0],
            along[l][1] - normal[l][0] + decay * carry[1],
        ]
    carry = [zero, zero]
    for l in reversed(range(layers)):
        down.append(carry)
        carry = [
            along[l][0] - normal[l][1] + decay * carry[0],
            along[l][1] + normal[l][0] + decay * carry[1],
        ]
    down = down[::-1]
    out = []
    for l in range(layers):
        psi = [rest * along[l][i] + near * (up[l][i] + down[l][i]) for i in range(2)]
        chi = [
            self_z * normal[l][0] - near * (up[l][1] - down[l][1]),
            self_z * normal[l][1] + near * (up[l][0] - down[l][0]),
        ]
        stiff = params[l, 1] * laplace
        below = RKKY_STRENGTH * params[l, 2]
        above = RKKY_STRENGTH * params[l, 3]
        comps = []
        for c in range(3):
            pair = []
            for i in range(2):
                value = -(unit_x * psi[i] if c == 0 else unit_y * psi[i] if c == 1 else chi[i])
                value = value + stiff * spectra[l][c][i]
                if l > 0:
                    value = value + below * spectra[l - 1][c][i]
                if l < layers - 1:
                    value = value + above * spectra[l + 1][c][i]
                pair.append(value)
            comps.append(pair)
        out.append(comps)
    return out


def spectral_kernel(layers, width, nx, ny, at_ref, params_ref, in_ref, out_ref):
    device = at_ref[0]
    block = pl.program_id(0)
    scale = 1.0 / (nx * ny)
    low, high = pl.ds(0, LANES), pl.ds(LANES, LANES)
    real, imag = pl.ds(0, width), pl.ds(width, width)

    def wave_y(shape):
        place = block * LANES + lax.broadcasted_iota(jnp.int32, shape, len(shape) - 1)
        nyquist = place == ny // 2
        signed = jnp.where(place < ny // 2, place, place - ny)
        return nyquist, 2.0 * math.pi / ny * signed.astype(jnp.float32)

    shape = (width, LANES)
    column = device * width + lax.broadcasted_iota(jnp.int32, shape, 0)
    generic = jnp.where(column == 0, 0.0, 1.0)
    weight = scale * (1.0 + generic)
    nyquist, rows_y = wave_y(shape)
    factors = plane(2.0 * math.pi / nx * column.astype(jnp.float32), rows_y)
    has_nyquist = block == ny // 2 // LANES

    def load():
        spectra = []
        for l in range(layers):
            comps = []
            for c in range(3):
                at = 3 * l + c
                comps.append(
                    [
                        in_ref[at, real, low] + generic * in_ref[at, imag, high],
                        generic * in_ref[at, imag, low] - in_ref[at, real, high],
                    ]
                )
            spectra.append(comps)
        return spectra

    def store(field):
        for l in range(layers):
            for c in range(3):
                at = 3 * l + c
                field_real = weight * field[l][c][0]
                field_imag = weight * field[l][c][1]
                out_ref[at, real, low] = field_real
                out_ref[at, real, high] = -field_imag
                out_ref[at, imag, low] = field_imag
                out_ref[at, imag, high] = field_real

    def mean_of(one, two):
        return [[[0.5 * (a + b) for a, b in zip(p, q)] for p, q in zip(u, v)] for u, v in zip(one, two)]

    @pl.when(jnp.logical_not(has_nyquist))
    def _():
        store(field_of(load(), factors, 1.0, 1.0, params_ref, layers))

    @pl.when(has_nyquist)
    def _():
        spectra = load()
        flip = jnp.where(nyquist, -1.0, 1.0)
        store(
            mean_of(
                field_of(spectra, factors, 1.0, 1.0, params_ref, layers),
                field_of(spectra, factors, 1.0, flip, params_ref, layers),
            )
        )

    @pl.when(device == 0)
    def _():
        line = (1, LANES)
        corner, line_y = wave_y(line)
        line_factors = plane(jnp.full(line, -math.pi, jnp.float32), line_y)
        row = pl.ds(width, 1)
        spectra = [
            [[in_ref[3 * l + c, row, low], -in_ref[3 * l + c, row, high]] for c in range(3)]
            for l in range(layers)
        ]
        flip = jnp.where(corner, -1.0, 1.0)
        field = mean_of(
            field_of(spectra, line_factors, 1.0, 1.0, params_ref, layers),
            field_of(spectra, line_factors, -1.0, flip, params_ref, layers),
        )
        for l in range(layers):
            for c in range(3):
                out_ref[3 * l + c, row, low] = scale * field[l][c][0]
                out_ref[3 * l + c, row, high] = -scale * field[l][c][1]


def spectral_field(spectra, params, device, nx, ny):
    layers = params.shape[0]
    lead, pair, length = spectra.shape
    block = (lead, pair, 2 * LANES)
    return pl.pallas_call(
        functools.partial(spectral_kernel, layers, pair // 2, nx, ny),
        out_shape=jax.ShapeDtypeStruct(spectra.shape, jnp.float32),
        grid=(length // (2 * LANES),),
        in_specs=[
            pl.BlockSpec(memory_space=pltpu.SMEM),
            pl.BlockSpec(memory_space=pltpu.SMEM),
            pl.BlockSpec(block, lambda i: (0, 0, i)),
        ],
        out_specs=pl.BlockSpec(block, lambda i: (0, 0, i)),
        cost_estimate=pl.CostEstimate(flops=60 * spectra.size, bytes_accessed=8 * spectra.size, transcendentals=0),
        name="spectral_field",
    )(device, params, spectra)


def cross_product(one, two):
    return [
        one[1] * two[2] - one[2] * two[1],
        one[2] * two[0] - one[0] * two[2],
        one[0] * two[1] - one[1] * two[0],
    ]


def on_device(magnet, saturation, stiffness, damping, interface_sign):
    axes = ("layer", "row")
    layers, bands = lax.axis_size("layer"), lax.axis_size("row")
    devices = layers * bands
    rows, nx = magnet.shape[2], magnet.shape[3]
    ny = rows * bands
    pair = nx // devices
    own = jnp.concatenate(
        [saturation[:, None], stiffness[:, None], interface_sign.astype(jnp.float32)], axis=1
    )
    params = lax.all_gather(own, "layer", axis=0, tiled=True)
    device = (lax.axis_index("layer") * bands + lax.axis_index("row")).reshape(1)
    flat = magnet.reshape(3 * rows, nx)
    table_x = x_table(nx, devices)
    table_y = y_table(ny)
    half = lax.dot_general(table_x, flat, (((1,), (1,)), ((), ())), precision=HIGH)
    sent = half.reshape(devices, pair, 3 * rows)
    got = lax.all_to_all(sent, axes, split_axis=0, concat_axis=0, tiled=True)
    got = got.reshape(layers, bands, pair, 3, rows).transpose(0, 3, 2, 1, 4)
    got = got.reshape(layers * 3 * pair, ny)
    spectra = lax.dot_general(got, table_y, (((1,), (0,)), ((), ())), precision=HIGH)
    field = spectral_field(spectra.reshape(layers * 3, pair, 2 * ny), params, device, nx, ny)
    back = lax.dot_general(
        field.reshape(layers * 3 * pair, 2 * ny), table_y, (((1,), (1,)), ((), ())), precision=HIGH
    )
    back = back.reshape(layers, 3, pair, bands, rows).transpose(0, 3, 2, 1, 4)
    back = back.reshape(devices, pair, 3 * rows)
    home = lax.all_to_all(back, axes, split_axis=0, concat_axis=0, tiled=True)
    total = lax.dot_general(
        home.reshape(nx, 3 * rows), table_x, (((0,), (0,)), ((), ())), precision=HIGH
    )
    total = total.reshape(3, rows, nx)
    spin = magnet.reshape(3, rows, nx)
    precess = cross_product(spin, total)
    relax = cross_product(spin, precess)
    damp = damping[0]
    factor = -1.0 / (1.0 + damp * damp)
    torque = jnp.stack([factor * (p + damp * q) for p, q in zip(precess, relax)])
    return torque.reshape(magnet.shape)


def solution(mesh):
    in_specs = (P(None, "layer", "row", None), P("layer"), P("layer"), P("layer"), P("layer", None))
    out_specs = P(None, "layer", "row", None)
    return jax.shard_map(
        on_device, mesh=mesh, in_specs=in_specs, out_specs=out_specs, check_vma=False
    )
```

```python
import functools
import math

import jax
import jax.numpy as jnp
import numpy as np
from jax import lax
from jax.experimental import pallas as pl
from jax.experimental.pallas import tpu as pltpu
from jax.sharding import PartitionSpec as P

THICKNESS = 1.0
LAYER_PITCH = 1.5
RKKY_STRENGTH = 0.8
HIGH = lax.Precision.HIGH
LANES = 128
CHUNKS = 2


def angle_pair(phase):
    return np.cos(phase).astype(np.float32), np.sin(phase).astype(np.float32)


def turn(first, second, modulus):
    return 2.0 * math.pi / modulus * (np.outer(first, second) % modulus)


def outer_cosine(angle_one, angle_two):
    cos_one, sin_one = angle_pair(angle_one)
    cos_two, sin_two = angle_pair(angle_two)
    table = cos_one[:, None] * jnp.asarray(cos_two)[None] - sin_one[:, None] * jnp.asarray(sin_two)[None]
    return table.reshape(-1, table.shape[2])


def x_table(length, devices, chunk, chunks):
    width = length // 2 // devices
    part = width // chunks
    points = np.arange(length)
    base = turn(width * np.arange(devices), points, length)
    step = turn(chunk * part + np.arange(part), points, length)
    table = outer_cosine(base, np.concatenate([step, step + math.pi / 2]))
    if chunk > 0:
        return table
    rows = lax.broadcasted_iota(jnp.int32, table.shape, 0)
    odd = lax.broadcasted_iota(jnp.int32, table.shape, 1) % 2
    return jnp.where(rows == part, 1.0 - 2.0 * odd.astype(jnp.float32), table)


def y_table(length):
    freq = np.arange(length).reshape(-1, 1, LANES)
    freq = np.broadcast_to(freq, (length // LANES, 2, LANES)).reshape(-1)
    shift = np.broadcast_to(np.array([0.0, math.pi / 2])[None, :, None], (length // LANES, 2, LANES)).reshape(-1)
    fine = 32
    coarse = turn(fine * np.arange(length // fine), freq, length) - shift[None]
    return outer_cosine(coarse, turn(np.arange(fine), freq, length))


def plane(wave_x, wave_y):
    square = wave_x * wave_x + wave_y * wave_y
    anchor = square == 0.0
    norm = jnp.sqrt(jnp.where(anchor, 1.0, square))
    unit_x = jnp.where(anchor, 0.0, wave_x / norm)
    unit_y = jnp.where(anchor, 0.0, wave_y / norm)
    depth = THICKNESS * norm
    series = 1.0 - depth / 11.0
    for term in range(10, 2, -1):
        series = 1.0 - depth / term * series
    rest = jnp.where(depth < 0.5, 0.5 * depth * series, 1.0 - (1.0 - jnp.exp(-depth)) / depth)
    rest = jnp.where(anchor, 0.0, rest)
    self_z = 1.0 - rest
    form = jnp.where(anchor, 0.0, 0.5 * depth * self_z * self_z)
    near = form * jnp.exp(-norm * (LAYER_PITCH - THICKNESS))
    decay = jnp.exp(-norm * LAYER_PITCH)
    laplace = 2.0 * jnp.cos(wave_x) + 2.0 * jnp.cos(wave_y) - 4.0
    return unit_x, unit_y, rest, self_z, near, decay, laplace


def field_of(spectra, factors, sign_x, sign_y, param, layers):
    unit_x, unit_y, rest, self_z, near, decay, laplace = factors
    unit_x = unit_x * sign_x
    unit_y = unit_y * sign_y
    along, normal, up, down = [], [], [], []
    for l in range(layers):
        moment = param(l, 0)
        along.append([moment * (unit_x * spectra[l][0][i] + unit_y * spectra[l][1][i]) for i in range(2)])
        normal.append([moment * spectra[l][2][i] for i in range(2)])
    zero = jnp.zeros_like(along[0][0])
    carry = [zero, zero]
    for l in range(layers):
        up.append(carry)
        carry = [
            along[l][0] + normal[l][1] + decay * carry[0],
            along[l][1] - normal[l][0] + decay * carry[1],
        ]
    carry = [zero, zero]
    for l in reversed(range(layers)):
        down.append(carry)
        carry = [
            along[l][0] - normal[l][1] + decay * carry[0],
            along[l][1] + normal[l][0] + decay * carry[1],
        ]
    down = down[::-1]
    out = []
    for l in range(layers):
        psi = [rest * along[l][i] + near * (up[l][i] + down[l][i]) for i in range(2)]
        chi = [
            self_z * normal[l][0] - near * (up[l][1] - down[l][1]),
            self_z * normal[l][1] + near * (up[l][0] - down[l][0]),
        ]
        stiff = param(l, 1) * laplace
        below = RKKY_STRENGTH * param(l, 2)
        above = RKKY_STRENGTH * param(l, 3)
        comps = []
        for c in range(3):
            pair = []
            for i in range(2):
                value = -(unit_x * psi[i] if c == 0 else unit_y * psi[i] if c == 1 else chi[i])
                value = value + stiff * spectra[l][c][i]
                if l > 0:
                    value = value + below * spectra[l - 1][c][i]
                if l < layers - 1:
                    value = value + above * spectra[l + 1][c][i]
                pair.append(value)
            comps.append(pair)
        out.append(comps)
    return out


def spectral_kernel(layers, width, chunk, chunks, nx, ny, at_ref, params_ref, in_ref, out_ref):
    device, layer = at_ref[0], at_ref[1]

    def param(l, which):
        return params_ref[lax.rem(layer + layers - l, layers), which]

    block = pl.program_id(0)
    scale = 1.0 / (nx * ny)
    low, high = pl.ds(0, LANES), pl.ds(LANES, LANES)
    real, imag = pl.ds(0, width), pl.ds(width, width)

    def wave_y(shape):
        place = block * LANES + lax.broadcasted_iota(jnp.int32, shape, len(shape) - 1)
        nyquist = place == ny // 2
        signed = jnp.where(place < ny // 2, place, place - ny)
        return nyquist, 2.0 * math.pi / ny * signed.astype(jnp.float32)

    shape = (width, LANES)
    column = (device * chunks + chunk) * width + lax.broadcasted_iota(jnp.int32, shape, 0)
    generic = jnp.where(column == 0, 0.0, 1.0)
    weight = scale * (1.0 + generic)
    nyquist, rows_y = wave_y(shape)
    factors = plane(2.0 * math.pi / nx * column.astype(jnp.float32), rows_y)
    has_nyquist = block == ny // 2 // LANES

    def load():
        spectra = []
        for l in range(layers):
            comps = []
            for c in range(3):
                at = 3 * l + c
                comps.append(
                    [
                        in_ref[at, real, low] + generic * in_ref[at, imag, high],
                        generic * in_ref[at, imag, low] - in_ref[at, real, high],
                    ]
                )
            spectra.append(comps)
        return spectra

    def store(field):
        for l in range(layers):
            for c in range(3):
                at = 3 * l + c
                field_real = weight * field[l][c][0]
                field_imag = weight * field[l][c][1]
                out_ref[at, real, low] = field_real
                out_ref[at, real, high] = -field_imag
                out_ref[at, imag, low] = field_imag
                out_ref[at, imag, high] = field_real

    def mean_of(one, two):
        return [[[0.5 * (a + b) for a, b in zip(p, q)] for p, q in zip(u, v)] for u, v in zip(one, two)]

    @pl.when(jnp.logical_not(has_nyquist))
    def _():
        store(field_of(load(), factors, 1.0, 1.0, param, layers))

    @pl.when(has_nyquist)
    def _():
        spectra = load()
        flip = jnp.where(nyquist, -1.0, 1.0)
        store(
            mean_of(
                field_of(spectra, factors, 1.0, 1.0, param, layers),
                field_of(spectra, factors, 1.0, flip, param, layers),
            )
        )

    if chunk > 0:
        return

    @pl.when(device == 0)
    def _():
        line = (1, LANES)
        corner, line_y = wave_y(line)
        line_factors = plane(jnp.full(line, -math.pi, jnp.float32), line_y)
        row = pl.ds(width, 1)
        spectra = [
            [[in_ref[3 * l + c, row, low], -in_ref[3 * l + c, row, high]] for c in range(3)]
            for l in range(layers)
        ]
        flip = jnp.where(corner, -1.0, 1.0)
        field = mean_of(
            field_of(spectra, line_factors, 1.0, 1.0, param, layers),
            field_of(spectra, line_factors, -1.0, flip, param, layers),
        )
        for l in range(layers):
            for c in range(3):
                out_ref[3 * l + c, row, low] = scale * field[l][c][0]
                out_ref[3 * l + c, row, high] = -scale * field[l][c][1]


def spectral_field(spectra, params, place, chunk, chunks, nx, ny):
    layers = params.shape[0]
    lead, pair, length = spectra.shape
    block = (lead, pair, 2 * LANES)
    return pl.pallas_call(
        functools.partial(spectral_kernel, layers, pair // 2, chunk, chunks, nx, ny),
        out_shape=jax.ShapeDtypeStruct(spectra.shape, jnp.float32),
        grid=(length // (2 * LANES),),
        in_specs=[
            pl.BlockSpec(memory_space=pltpu.SMEM),
            pl.BlockSpec(memory_space=pltpu.SMEM),
            pl.BlockSpec(block, lambda i: (0, 0, i)),
        ],
        out_specs=pl.BlockSpec(block, lambda i: (0, 0, i)),
        cost_estimate=pl.CostEstimate(flops=60 * spectra.size, bytes_accessed=8 * spectra.size, transcendentals=0),
        name=f"spectral_field_{chunk}",
    )(place, params, spectra)


def cross_product(one, two):
    return [
        one[1] * two[2] - one[2] * two[1],
        one[2] * two[0] - one[0] * two[2],
        one[0] * two[1] - one[1] * two[0],
    ]


def on_device(magnet, saturation, stiffness, damping, interface_sign):
    axes = ("layer", "row")
    layers, bands = lax.axis_size("layer"), lax.axis_size("row")
    devices = layers * bands
    rows, nx = magnet.shape[2], magnet.shape[3]
    ny = rows * bands
    chunks = CHUNKS
    while (nx // 2 // devices) % chunks:
        chunks -= 1
    pair = nx // devices // chunks
    own = jnp.concatenate(
        [saturation[:, None], stiffness[:, None], interface_sign.astype(jnp.float32)], axis=1
    )
    shifted = [own]
    for step in range(1, layers):
        shifted.append(lax.ppermute(own, "layer", [(i, (i + step) % layers) for i in range(layers)]))
    params = jnp.concatenate(shifted, axis=0)
    layer = lax.axis_index("layer")
    place = jnp.stack([layer * bands + lax.axis_index("row"), layer])
    flat = magnet.reshape(3 * rows, nx)
    tables = [x_table(nx, devices, chunk, chunks) for chunk in range(chunks)]
    table_y = y_table(ny)
    arrived = []
    for table in tables:
        half = lax.dot_general(table, flat, (((1,), (1,)), ((), ())), precision=HIGH)
        sent = half.reshape(devices, pair, 3 * rows)
        arrived.append(lax.all_to_all(sent, axes, split_axis=0, concat_axis=0, tiled=True))
    total = None
    for chunk, got in enumerate(arrived):
        got = got.reshape(layers, bands, pair, 3, rows).transpose(0, 3, 2, 1, 4)
        got = got.reshape(layers * 3 * pair, ny)
        spectra = lax.dot_general(got, table_y, (((1,), (0,)), ((), ())), precision=HIGH)
        spectra = spectra.reshape(layers * 3, pair, 2 * ny)
        field = spectral_field(spectra, params, place, chunk, chunks, nx, ny)
        back = lax.dot_general(
            field.reshape(layers * 3 * pair, 2 * ny), table_y, (((1,), (1,)), ((), ())), precision=HIGH
        )
        back = back.reshape(layers, 3, pair, bands, rows).transpose(0, 3, 2, 1, 4)
        back = back.reshape(devices, pair, 3 * rows)
        home = lax.all_to_all(back, axes, split_axis=0, concat_axis=0, tiled=True)
        piece = lax.dot_general(
            home.reshape(devices * pair, 3 * rows), tables[chunk], (((0,), (0,)), ((), ())), precision=HIGH
        )
        total = piece if total is None else total + piece
    total = total.reshape(3, rows, nx)
    spin = magnet.reshape(3, rows, nx)
    precess = cross_product(spin, total)
    relax = cross_product(spin, precess)
    damp = damping[0]
    factor = -1.0 / (1.0 + damp * damp)
    torque = jnp.stack([factor * (p + damp * q) for p, q in zip(precess, relax)])
    return torque.reshape(magnet.shape)


def solution(mesh):
    in_specs = (P(None, "layer", "row", None), P("layer"), P("layer"), P("layer"), P("layer", None))
    out_specs = P(None, "layer", "row", None)
    return jax.shard_map(
        on_device, mesh=mesh, in_specs=in_specs, out_specs=out_specs, check_vma=False
    )
```

```python
import functools
import math

import jax
import jax.numpy as jnp
import numpy as np
from jax import lax
from jax.experimental import pallas as pl
from jax.experimental.pallas import tpu as pltpu
from jax.sharding import PartitionSpec as P

THICKNESS = 1.0
LAYER_PITCH = 1.5
RKKY_STRENGTH = 0.8
HIGH = lax.Precision.HIGH
LANES = 128
CHUNKS = 2


def angle_pair(phase):
    return np.cos(phase).astype(np.float32), np.sin(phase).astype(np.float32)


def turn(first, second, modulus):
    return 2.0 * math.pi / modulus * (np.outer(first, second) % modulus)


def seeds_of(angle_one, angle_two):
    return [jnp.asarray(part) for part in angle_pair(angle_one) + angle_pair(angle_two)]


def outer_product(seeds):
    cos_one, sin_one, cos_two, sin_two = seeds
    table = cos_one[:, None] * cos_two[None] - sin_one[:, None] * sin_two[None]
    return table.reshape(-1, table.shape[2])


def x_table(length, devices, chunk, chunks):
    width = length // 2 // devices
    part = width // chunks
    points = np.arange(length)
    base = turn(width * np.arange(devices), points, length)
    step = turn(chunk * part + np.arange(part), points, length)
    table = outer_product(seeds_of(base, np.concatenate([step, step + math.pi / 2])))
    if chunk > 0:
        return table
    rows = lax.broadcasted_iota(jnp.int32, table.shape, 0)
    odd = lax.broadcasted_iota(jnp.int32, table.shape, 1) % 2
    return jnp.where(rows == part, 1.0 - 2.0 * odd.astype(jnp.float32), table)


def y_seeds(length):
    freq = np.arange(length).reshape(-1, 1, LANES)
    freq = np.broadcast_to(freq, (length // LANES, 2, LANES)).reshape(-1)
    shift = np.broadcast_to(np.array([0.0, math.pi / 2])[None, :, None], (length // LANES, 2, LANES)).reshape(-1)
    fine = 32
    coarse = turn(fine * np.arange(length // fine), freq, length) - shift[None]
    return seeds_of(coarse, turn(np.arange(fine), freq, length))


def plane(wave_x, wave_y):
    square = wave_x * wave_x + wave_y * wave_y
    anchor = square == 0.0
    norm = jnp.sqrt(jnp.where(anchor, 1.0, square))
    unit_x = jnp.where(anchor, 0.0, wave_x / norm)
    unit_y = jnp.where(anchor, 0.0, wave_y / norm)
    depth = THICKNESS * norm
    series = 1.0 - depth / 11.0
    for term in range(10, 2, -1):
        series = 1.0 - depth / term * series
    rest = jnp.where(depth < 0.5, 0.5 * depth * series, 1.0 - (1.0 - jnp.exp(-depth)) / depth)
    rest = jnp.where(anchor, 0.0, rest)
    self_z = 1.0 - rest
    form = jnp.where(anchor, 0.0, 0.5 * depth * self_z * self_z)
    near = form * jnp.exp(-norm * (LAYER_PITCH - THICKNESS))
    decay = jnp.exp(-norm * LAYER_PITCH)
    laplace = 2.0 * jnp.cos(wave_x) + 2.0 * jnp.cos(wave_y) - 4.0
    return unit_x, unit_y, rest, self_z, near, decay, laplace


def field_of(spectra, factors, sign_x, sign_y, param, layers):
    unit_x, unit_y, rest, self_z, near, decay, laplace = factors
    unit_x = unit_x * sign_x
    unit_y = unit_y * sign_y
    along, normal, up, down = [], [], [], []
    for l in range(layers):
        moment = param(l, 0)
        along.append([moment * (unit_x * spectra[l][0][i] + unit_y * spectra[l][1][i]) for i in range(2)])
        normal.append([moment * spectra[l][2][i] for i in range(2)])
    zero = jnp.zeros_like(along[0][0])
    carry = [zero, zero]
    for l in range(layers):
        up.append(carry)
        carry = [
            along[l][0] + normal[l][1] + decay * carry[0],
            along[l][1] - normal[l][0] + decay * carry[1],
        ]
    carry = [zero, zero]
    for l in reversed(range(layers)):
        down.append(carry)
        carry = [
            along[l][0] - normal[l][1] + decay * carry[0],
            along[l][1] + normal[l][0] + decay * carry[1],
        ]
    down = down[::-1]
    out = []
    for l in range(layers):
        psi = [rest * along[l][i] + near * (up[l][i] + down[l][i]) for i in range(2)]
        chi = [
            self_z * normal[l][0] - near * (up[l][1] - down[l][1]),
            self_z * normal[l][1] + near * (up[l][0] - down[l][0]),
        ]
        stiff = param(l, 1) * laplace
        below = RKKY_STRENGTH * param(l, 2)
        above = RKKY_STRENGTH * param(l, 3)
        comps = []
        for c in range(3):
            pair = []
            for i in range(2):
                value = -(unit_x * psi[i] if c == 0 else unit_y * psi[i] if c == 1 else chi[i])
                value = value + stiff * spectra[l][c][i]
                if l > 0:
                    value = value + below * spectra[l - 1][c][i]
                if l < layers - 1:
                    value = value + above * spectra[l + 1][c][i]
                pair.append(value)
            comps.append(pair)
        out.append(comps)
    return out


def spectral_kernel(layers, width, chunk, chunks, nx, ny, at_ref, params_ref, in_ref, out_ref):
    device, layer = at_ref[0], at_ref[1]

    def param(l, which):
        return params_ref[lax.rem(layer + layers - l, layers), which]

    block = pl.program_id(0)
    scale = 1.0 / (nx * ny)
    low, high = pl.ds(0, LANES), pl.ds(LANES, LANES)
    real, imag = pl.ds(0, width), pl.ds(width, width)

    def wave_y(shape):
        place = block * LANES + lax.broadcasted_iota(jnp.int32, shape, len(shape) - 1)
        nyquist = place == ny // 2
        signed = jnp.where(place < ny // 2, place, place - ny)
        return nyquist, 2.0 * math.pi / ny * signed.astype(jnp.float32)

    shape = (width, LANES)
    column = (device * chunks + chunk) * width + lax.broadcasted_iota(jnp.int32, shape, 0)
    generic = jnp.where(column == 0, 0.0, 1.0)
    weight = scale * (1.0 + generic)
    nyquist, rows_y = wave_y(shape)
    factors = plane(2.0 * math.pi / nx * column.astype(jnp.float32), rows_y)
    has_nyquist = block == ny // 2 // LANES

    def load():
        spectra = []
        for l in range(layers):
            comps = []
            for c in range(3):
                at = 3 * l + c
                comps.append(
                    [
                        in_ref[at, real, low] + generic * in_ref[at, imag, high],
                        generic * in_ref[at, imag, low] - in_ref[at, real, high],
                    ]
                )
            spectra.append(comps)
        return spectra

    def store(field):
        for l in range(layers):
            for c in range(3):
                at = 3 * l + c
                field_real = weight * field[l][c][0]
                field_imag = weight * field[l][c][1]
                out_ref[at, real, low] = field_real
                out_ref[at, real, high] = -field_imag
                out_ref[at, imag, low] = field_imag
                out_ref[at, imag, high] = field_real

    def mean_of(one, two):
        return [[[0.5 * (a + b) for a, b in zip(p, q)] for p, q in zip(u, v)] for u, v in zip(one, two)]

    @pl.when(jnp.logical_not(has_nyquist))
    def _():
        store(field_of(load(), factors, 1.0, 1.0, param, layers))

    @pl.when(has_nyquist)
    def _():
        spectra = load()
        flip = jnp.where(nyquist, -1.0, 1.0)
        store(
            mean_of(
                field_of(spectra, factors, 1.0, 1.0, param, layers),
                field_of(spectra, factors, 1.0, flip, param, layers),
            )
        )

    if chunk > 0:
        return

    @pl.when(device == 0)
    def _():
        line = (1, LANES)
        corner, line_y = wave_y(line)
        line_factors = plane(jnp.full(line, -math.pi, jnp.float32), line_y)
        row = pl.ds(width, 1)
        spectra = [
            [[in_ref[3 * l + c, row, low], -in_ref[3 * l + c, row, high]] for c in range(3)]
            for l in range(layers)
        ]
        flip = jnp.where(corner, -1.0, 1.0)
        field = mean_of(
            field_of(spectra, line_factors, 1.0, 1.0, param, layers),
            field_of(spectra, line_factors, -1.0, flip, param, layers),
        )
        for l in range(layers):
            for c in range(3):
                out_ref[3 * l + c, row, low] = scale * field[l][c][0]
                out_ref[3 * l + c, row, high] = -scale * field[l][c][1]


def spectral_field(spectra, params, place, chunk, chunks, nx, ny):
    layers = params.shape[0]
    lead, pair, length = spectra.shape
    block = (lead, pair, 2 * LANES)
    return pl.pallas_call(
        functools.partial(spectral_kernel, layers, pair // 2, chunk, chunks, nx, ny),
        out_shape=jax.ShapeDtypeStruct(spectra.shape, jnp.float32),
        grid=(length // (2 * LANES),),
        in_specs=[
            pl.BlockSpec(memory_space=pltpu.SMEM),
            pl.BlockSpec(memory_space=pltpu.SMEM),
            pl.BlockSpec(block, lambda i: (0, 0, i)),
        ],
        out_specs=pl.BlockSpec(block, lambda i: (0, 0, i)),
        cost_estimate=pl.CostEstimate(flops=60 * spectra.size, bytes_accessed=8 * spectra.size, transcendentals=0),
    )(place, params, spectra)


def gather_kernel(bands, rows, in_ref, out_ref):
    for c in range(3):
        out_ref[c] = jnp.concatenate([in_ref[b, :, c * rows : (c + 1) * rows] for b in range(bands)], axis=-1)


def scatter_kernel(bands, rows, in_ref, out_ref):
    for b in range(bands):
        out_ref[b] = jnp.concatenate([in_ref[c, :, b * rows : (b + 1) * rows] for c in range(3)], axis=-1)


def relayout(kernel, values, lead_in, lead_out, bands, rows):
    pair = values.shape[1]
    blocks = values.shape[0] // lead_in
    out_width = rows * lead_in
    return pl.pallas_call(
        functools.partial(kernel, bands, rows),
        out_shape=jax.ShapeDtypeStruct((blocks * lead_out, pair, out_width), jnp.float32),
        grid=(blocks,),
        in_specs=[pl.BlockSpec((lead_in, pair, values.shape[2]), lambda i: (i, 0, 0))],
        out_specs=pl.BlockSpec((lead_out, pair, out_width), lambda i: (i, 0, 0)),
        cost_estimate=pl.CostEstimate(flops=0, bytes_accessed=8 * values.size, transcendentals=0),
    )(values)


def cross_product(one, two):
    return [
        one[1] * two[2] - one[2] * two[1],
        one[2] * two[0] - one[0] * two[2],
        one[0] * two[1] - one[1] * two[0],
    ]


def step(magnet, saturation, stiffness, damping, interface_sign):
    axes = ("layer", "row")
    layers, bands = lax.axis_size("layer"), lax.axis_size("row")
    devices = layers * bands
    rows, nx = magnet.shape[2], magnet.shape[3]
    ny = rows * bands
    chunks = CHUNKS
    while (nx // 2 // devices) % chunks:
        chunks -= 1
    pair = nx // devices // chunks
    own = jnp.concatenate(
        [saturation[:, None], stiffness[:, None], interface_sign.astype(jnp.float32)], axis=1
    )
    layer = lax.axis_index("layer")
    place = jnp.stack([layer * bands + lax.axis_index("row"), layer])
    flat = magnet.reshape(3 * rows, nx)
    tables = [x_table(nx, devices, chunk, chunks) for chunk in range(chunks)]
    seeds = y_seeds(ny)
    arrived = []
    for chunk, table in enumerate(tables):
        half = lax.dot_general(table, flat, (((1,), (1,)), ((), ())), precision=HIGH)
        if chunk == 0:
            half, own, seeds = lax.optimization_barrier((half, own, seeds))
            shifted = [own]
            for hop in range(1, layers):
                shifted.append(lax.ppermute(own, "layer", [(i, (i + hop) % layers) for i in range(layers)]))
            params = jnp.concatenate(shifted, axis=0)
            seeds, params = lax.optimization_barrier((seeds, params))
            table_y = lax.optimization_barrier(outer_product(seeds))
        sent = half.reshape(devices, pair, 3 * rows)
        arrived.append(lax.all_to_all(sent, axes, split_axis=0, concat_axis=0, tiled=True))
    total = None
    for chunk, got in enumerate(arrived):
        got = relayout(gather_kernel, got, bands, 3, bands, rows)
        got = got.reshape(layers * 3 * pair, ny)
        spectra = lax.dot_general(got, table_y, (((1,), (0,)), ((), ())), precision=HIGH)
        spectra = spectra.reshape(layers * 3, pair, 2 * ny)
        field = spectral_field(spectra, params, place, chunk, chunks, nx, ny)
        back = lax.dot_general(
            field.reshape(layers * 3 * pair, 2 * ny), table_y, (((1,), (1,)), ((), ())), precision=HIGH
        )
        back = back.reshape(layers * 3, pair, ny)
        back = relayout(scatter_kernel, back, 3, bands, bands, rows)
        home = lax.all_to_all(back, axes, split_axis=0, concat_axis=0, tiled=True)
        piece = lax.dot_general(
            home.reshape(devices * pair, 3 * rows), tables[chunk], (((0,), (0,)), ((), ())), precision=HIGH
        )
        total = piece if total is None else total + piece
    total = total.reshape(3, rows, nx)
    spin = magnet.reshape(3, rows, nx)
    precess = cross_product(spin, total)
    relax = cross_product(spin, precess)
    damp = damping[0]
    factor = -1.0 / (1.0 + damp * damp)
    torque = jnp.stack([factor * (p + damp * q) for p, q in zip(precess, relax)])
    return torque.reshape(magnet.shape)


def solution(mesh):
    in_specs = (P(None, "layer", "row", None), P("layer"), P("layer"), P("layer"), P("layer", None))
    out_specs = P(None, "layer", "row", None)
    return jax.shard_map(step, mesh=mesh, in_specs=in_specs, out_specs=out_specs, check_vma=False)
```
